512 devices in a mesh: row: 32 (over z, y_hi, core), col: 16 (over y_lo, x).
Axes of the slice: x: 4, y: 8 (y_hi: 2, y_lo: 4; y = y_hi * 4 + y_lo), z: 8, core: 2. Of those that a mesh axis runs over, the one named last changes fastest.
Arguments:
- energy: float32 [16, 2048, 2048], P('col', 'row'), may hold values from 0.5 to 8
- damage_old: float32 [16, 2048, 2048], P('col', 'row'), may hold values from 0 to 0.8
- crack_seeds: int32 [16, 2048, 2048], P('col', 'row'), may hold values 0 or 1
- irreversible: int32 [16, 2048, 2048], P('col', 'row'), may hold values 0 or 1
- line_inverses: float32 [8, 256, 256], replicated, may hold values from -0.6 to 2.8
- z_inverse: float32 [16, 16], replicated, may hold values from -0.8 to 1.9
Outputs:
- damage: float32 [16, 2048, 2048], P('col', 'row')
- update_norms: float32 [2], replicated
The draws below stay inside these ranges and needn't reach their ends.
All inputs are finite; a program needn't handle non-finite values. No bound on the sum of `crack_seeds` or of `irreversible` on one device may be relied on, other than what follows from the above.
Results may differ from the reference program's by a relative error of at most 0.0001.
Values sent between devices are 32-bit elements; how exact they have to be, the bound alone decides.
No kernel may reach another device: no remote copies, remote signals or barrier semaphores. Data moves between devices by JAX's collectives and lax.ppermute only.
A program may use at most 64 MiB of HBM per device.

```python
import math
import jax
import jax.numpy as jnp
from jax import lax

L = 2048
BLK = 256
NBLK = 8
NZ = 16
ITERS = 2


def dominant_blocks(key, block_count, extent, low, high, spread):
    key_diag, key_rest = jax.random.split(key)
    diagonal = jax.random.uniform(key_diag, (block_count, extent), jnp.float32, low, high)
    scatter_part = spread * jax.random.truncated_normal(key_rest, -4.0, 4.0, (block_count, extent, extent), jnp.float32)
    return scatter_part + diagonal[:, :, None] * jnp.eye(extent, dtype=jnp.float32)[None]


def draw_line_inverses(key, part):
    return dominant_blocks(jax.random.fold_in(key, 11), NBLK, BLK, 1.0, 2.0, 0.5 / math.sqrt(BLK))


def draw_z_inverse(key, part):
    return dominant_blocks(jax.random.fold_in(key, 23), 1, NZ, 0.5, 1.0, 0.25 / math.sqrt(NZ))[0]


def plant(array, rng, low, top_value):
    index_at = [jax.random.randint(jax.random.fold_in(rng, axis), (), 0, length) for axis, length in enumerate(array.shape)]
    main_axis = array.shape.index(max(array.shape))
    next_to = index_at[:main_axis] + [(index_at[main_axis] + 1) % array.shape[main_axis]] + index_at[main_axis + 1:]
    return array.at[tuple(index_at)].set(low).at[tuple(next_to)].set(top_value)


def levels(rng, dims, pieces, smallest, high):
    loudness = 1.0
    for dim, blocks in pieces:
        steps = jax.random.uniform(jax.random.fold_in(jax.random.fold_in(rng, 6), dim), (blocks,), jnp.float32, smallest / len(pieces), high / len(pieces))
        loudness = loudness * jnp.repeat(jnp.exp(steps), dims[dim] // blocks).reshape((-1,) + (1,) * (len(dims) - 1 - dim))
    return loudness


def setup_inputs(seed: int = 0) -> dict:
    key_list = jax.random.split(jax.random.key(seed), 7)
    return {
        "energy": jnp.clip(jnp.exp(math.log(8.0) - 2.7725887 * jax.random.uniform(key_list[0], (NZ, L, L), jnp.float32) ** levels(key_list[0], (NZ, L, L), ((0, 16), (1, 32)), -0.2, 0.2)), 0.5, 8.0),
        "damage_old": jnp.clip(0.8 * jax.random.uniform(key_list[1], (NZ, L, L), jnp.float32) ** levels(key_list[1], (NZ, L, L), ((0, 16), (1, 32)), -0.2, 0.2), 0.0, 0.8),
        "crack_seeds": plant((jax.random.randint(key_list[2], (NZ, L, L), 0, 32) < 1).astype(jnp.int32), jax.random.fold_in(key_list[2], 1), 0, 1),
        "irreversible": plant((jax.random.randint(key_list[3], (NZ, L, L), 0, 2) < 1).astype(jnp.int32), jax.random.fold_in(key_list[3], 1), 0, 1),
        "line_inverses": draw_line_inverses(jax.random.fold_in(key_list[6], 71), 0),
        "z_inverse": draw_z_inverse(jax.random.fold_in(key_list[6], 71), 0),
    }


KAPPA = 2.0
STEP = 0.02
COUPLE = 0.5
EPSILON = 1e-06

def second_difference(grid_field, along):
    extent = grid_field.shape[along]
    forward_diff = lax.slice_in_dim(grid_field, 1, extent, axis=along) - lax.slice_in_dim(grid_field, 0, extent - 1, axis=along)
    zero_shape = list(grid_field.shape)
    zero_shape[along] = 1
    zero_rim = jnp.zeros(zero_shape, grid_field.dtype)
    ahead = jnp.concatenate([forward_diff, zero_rim], axis=along)
    behind = jnp.concatenate([zero_rim, forward_diff], axis=along)
    return ahead - behind

def line_solve(line_rows, inverses):
    block_count, block_cells, _ = inverses.shape
    line_count = line_rows.shape[0]
    blocks = line_rows.reshape(line_count, block_count, block_cells)
    products = jnp.einsum('rkb,kcb->rkc', blocks, inverses, precision=lax.Precision.HIGHEST)
    first_col = inverses[:, :, 0]
    last_col = inverses[:, :, block_cells - 1]
    incoming = [jnp.zeros((line_count,), line_rows.dtype)]
    for block_index in range(block_count - 1):
        incoming.append(products[:, block_index, block_cells - 1] + COUPLE * incoming[block_index] * inverses[block_index, block_cells - 1, 0])
    inflow = jnp.stack(incoming, axis=1)
    forward = products + COUPLE * inflow[:, :, None] * first_col[None]
    head_terms = [jnp.zeros((line_count,), line_rows.dtype) for block_index in range(block_count)]
    carried = forward[:, block_count - 1, 0]
    for block_index in range(block_count - 2, -1, -1):
        head_terms[block_index] = carried
        carried = forward[:, block_index, 0] + COUPLE * carried * inverses[block_index, 0, block_cells - 1]
    outflow = jnp.stack(head_terms, axis=1)
    solved = forward + COUPLE * outflow[:, :, None] * last_col[None]
    return solved.reshape(line_count, block_count * block_cells)

def reference(energy, damage_old, crack_seeds, irreversible, line_inverses, z_inverse):
    seeded = crack_seeds == 1
    damage = jnp.where(seeded, 1.0, damage_old)
    lower_bound = jnp.where(irreversible == 1, damage_old, 0.0)
    line_length = energy.shape[2]
    update_sizes = []
    for sweep_index in range(ITERS):
        laplace = second_difference(damage, 0) + second_difference(damage, 1) + second_difference(damage, 2)
        residual = energy - (1.0 + energy) * damage + KAPPA * laplace
        along_x = line_solve(residual.reshape(-1, line_length), line_inverses).reshape(residual.shape)
        turned = jnp.swapaxes(along_x, 1, 2)
        along_y = line_solve(turned.reshape(-1, line_length), line_inverses).reshape(turned.shape)
        along_z = jnp.einsum('zk,kxy->zxy', z_inverse, along_y, precision=lax.Precision.HIGHEST)
        update = STEP * jnp.swapaxes(along_z, 1, 2)
        clamped = jnp.minimum(jnp.maximum(damage + update, lower_bound), 1.0)
        renewed = jnp.where(seeded, 1.0, clamped)
        update_sizes.append(jnp.sqrt(jnp.mean((renewed - damage) ** 2) + EPSILON) / STEP)
        damage = renewed
    return (damage, jnp.stack(update_sizes))
```

```python
import jax
import jax.numpy as jnp
from jax import lax
from jax.experimental import pallas as pl
from jax.experimental.pallas import tpu as pltpu
from jax.sharding import Mesh
from jax.sharding import PartitionSpec as P

ROW = ("row_0", "row_1", "row_2")
COL = ("col_0", "col_1")
ALL = ROW + COL

KAPPA = 2.0
STEP = 0.02
COUPLE = 0.5
EPSILON = 1e-06
HALF = 64


def iota(shape, axis):
    return lax.broadcasted_iota(jnp.int32, shape, axis)


def lane_lap(field):
    extent = field.shape[1]
    lane = iota(field.shape, 1)
    ahead = jnp.where(lane == extent - 1, field, pltpu.roll(field, extent - 1, 1))
    behind = jnp.where(lane == 0, field, pltpu.roll(field, 1, 1))
    return (ahead - field) + (behind - field)


def plane_lap(field, planes):
    extent = field.shape[0]
    plane = iota(field.shape, 0) % planes
    ahead = jnp.where(plane == planes - 1, field, pltpu.roll(field, extent - 1, 0))
    behind = jnp.where(plane == 0, field, pltpu.roll(field, 1, 0))
    return (ahead - field) + (behind - field)


def line_solve(lines, inverses_ref):
    count = lines.shape[0]
    blocks, cells, _ = inverses_ref.shape
    unit_row = iota((8, cells), 0)
    unit_lane = iota((8, cells), 1)
    units = jnp.where(
        ((unit_row == 0) & (unit_lane == 0)) | ((unit_row == 1) & (unit_lane == cells - 1)), 1.0, 0.0
    )
    products, firsts, lasts = [], [], []
    for k in range(blocks):
        stacked = jnp.concatenate([lines[:, k * cells : (k + 1) * cells], units], axis=0)
        result = lax.dot_general(
            stacked,
            inverses_ref[k],
            (((1,), (1,)), ((), ())),
            precision=lax.Precision.HIGHEST,
            preferred_element_type=jnp.float32,
        )
        products.append(result[:count])
        firsts.append(result[count : count + 1])
        lasts.append(result[count + 1 : count + 2])
    inflow = [jnp.zeros((count, 1), jnp.float32)]
    heads = []
    for k in range(blocks):
        heads.append(products[k][:, 0:1] + COUPLE * inflow[k] * firsts[k][:, 0:1])
        if k < blocks - 1:
            inflow.append(
                products[k][:, cells - 1 : cells] + COUPLE * inflow[k] * firsts[k][:, cells - 1 : cells]
            )
    outflow = [None] * blocks
    carried = heads[blocks - 1]
    for k in range(blocks - 2, -1, -1):
        outflow[k] = carried
        carried = heads[k] + COUPLE * carried * lasts[k][:, 0:1]
    solved = []
    for k in range(blocks):
        value = products[k]
        if k > 0:
            value = value + (COUPLE * inflow[k]) * firsts[k]
        if k < blocks - 1:
            value = value + (COUPLE * outflow[k]) * lasts[k]
        solved.append(value)
    return jnp.concatenate(solved, axis=1)


def send_rows(out_ref, field, first, stride):
    chunks = field.shape[1] // 4
    for s in range(2):
        pair = jnp.concatenate(
            [field[:, 2 * s * chunks : (2 * s + 1) * chunks], field[:, (2 * s + 1) * chunks : (2 * s + 2) * chunks]],
            axis=0,
        )
        out_ref[pl.ds(first + s, chunks, stride=stride), :] = pair.T


def receive_rows(in_ref):
    chunks = in_ref.shape[0] // 2
    parts = []
    for s in range(2):
        pair = in_ref[pl.ds(s, chunks, stride=2), :].T
        parts.append(pair[:HALF])
        parts.append(pair[HALF:])
    return jnp.concatenate(parts, axis=1)


def partial_residual(energy, damage):
    return energy - (1.0 + energy) * damage + KAPPA * lane_lap(damage)


def first_kernel(energy_ref, old_ref, seeds_ref, out_ref):
    energy = energy_ref[0]
    damage = jnp.where(seeds_ref[0] == 1, 1.0, old_ref[0])
    send_rows(out_ref, damage, 2, 4)
    send_rows(out_ref, partial_residual(energy, damage), 0, 4)


def cross_kernel(in_ref, inverses_ref, z_ref, out_ref):
    planes = z_ref.shape[0]
    rows = in_ref.shape[0] // (4 * planes)
    low = iota((planes, 2 * HALF), 1) < HALF

    def gather(first):
        lines = [[], [], [], []]
        for j in range(rows // 2):
            for s in range(2):
                even = in_ref[pl.ds(2 * j * 4 * planes + first + s, planes, stride=4), :]
                odd = in_ref[pl.ds((2 * j + 1) * 4 * planes + first + s, planes, stride=4), :]
                lines[2 * s].append(jnp.where(low, even, pltpu.roll(odd, HALF, 1)))
                lines[2 * s + 1].append(jnp.where(low, pltpu.roll(even, HALF, 1), odd))
        return jnp.concatenate([jnp.concatenate(line, axis=1) for line in lines], axis=0)

    damage = gather(2)
    turned = gather(0) + KAPPA * (lane_lap(damage) + plane_lap(damage, planes))
    along_y = line_solve(turned, inverses_ref)
    wide = jnp.concatenate([z_ref[...]] * 4, axis=1)
    tiled = jnp.concatenate([wide] * 4, axis=0)
    same = iota(tiled.shape, 0) // planes == iota(tiled.shape, 1) // planes
    along_z = jnp.dot(
        jnp.where(same, tiled, 0.0),
        along_y,
        precision=lax.Precision.HIGHEST,
        preferred_element_type=jnp.float32,
    )
    for j in range(rows // 2):
        for s in range(2):
            first = along_z[2 * s * planes : (2 * s + 1) * planes, j * 128 : (j + 1) * 128]
            second = along_z[(2 * s + 1) * planes : (2 * s + 2) * planes, j * 128 : (j + 1) * 128]
            out_ref[pl.ds(2 * j * 2 * planes + s, planes, stride=2), :] = jnp.where(
                low, first, pltpu.roll(second, HALF, 1)
            )
            out_ref[pl.ds((2 * j + 1) * 2 * planes + s, planes, stride=2), :] = jnp.where(
                low, pltpu.roll(first, HALF, 1), second
            )


def renew(in_ref, damage, old, seeds, irreversible, inverses_ref):
    update = STEP * line_solve(receive_rows(in_ref), inverses_ref)
    lower_bound = jnp.where(irreversible == 1, old, 0.0)
    clamped = jnp.minimum(jnp.maximum(damage + update, lower_bound), 1.0)
    renewed = jnp.where(seeds == 1, 1.0, clamped)
    change = jnp.sum((renewed - damage) ** 2)
    return renewed, change


def middle_kernel(
    in_ref, energy_ref, old_ref, seeds_ref, irreversible_ref, inverses_ref, out_ref, damage_ref, change_ref
):
    old = old_ref[0]
    seeds = seeds_ref[0]
    damage = jnp.where(seeds == 1, 1.0, old)
    renewed, change = renew(in_ref, damage, old, seeds, irreversible_ref[0], inverses_ref)
    damage_ref[0] = renewed
    send_rows(out_ref, renewed, 2, 4)
    send_rows(out_ref, partial_residual(energy_ref[0], renewed), 0, 4)
    change_ref[...] = jnp.full(change_ref.shape, change, jnp.float32)


def last_kernel(
    in_ref, damage_in_ref, old_ref, seeds_ref, irreversible_ref, inverses_ref, first_change_ref, damage_ref, change_ref
):
    renewed, change = renew(
        in_ref, damage_in_ref[0], old_ref[0], seeds_ref[0], irreversible_ref[0], inverses_ref
    )
    damage_ref[0] = renewed
    lane = iota(change_ref.shape, 1)
    change_ref[...] = jnp.where(lane == 0, first_change_ref[...], jnp.where(lane == 1, change, 0.0))


def call(kernel, outs, *args):
    return pl.pallas_call(
        kernel,
        out_shape=[jax.ShapeDtypeStruct(shape, jnp.float32) for shape in outs],
        in_specs=[pl.BlockSpec(memory_space=pltpu.VMEM) for _ in args],
        out_specs=[pl.BlockSpec(memory_space=pltpu.VMEM) for _ in outs],
        compiler_params=pltpu.CompilerParams(vmem_limit_bytes=48 * 1024 * 1024),
    )(*args)


def exchange(rows):
    return lax.all_to_all(rows, ALL, split_axis=0, concat_axis=0, tiled=True)


def local(energy, damage_old, crack_seeds, irreversible, line_inverses, z_inverse):
    planes, rows_here, line_length = energy.shape
    devices = lax.axis_size(ALL)
    cell_count = planes * rows_here * line_length * devices
    one = planes * rows_here * line_length // 128
    (sent,) = call(first_kernel, [(2 * one, 128)], energy, damage_old, crack_seeds)
    (crossed,) = call(cross_kernel, [(one, 128)], exchange(sent), line_inverses, z_inverse)
    sent, damage, change = call(
        middle_kernel,
        [(2 * one, 128), energy.shape, (1, 128)],
        exchange(crossed),
        energy,
        damage_old,
        crack_seeds,
        irreversible,
        line_inverses,
    )
    (crossed,) = call(cross_kernel, [(one, 128)], exchange(sent), line_inverses, z_inverse)
    damage, change = call(
        last_kernel,
        [energy.shape, (1, 128)],
        exchange(crossed),
        damage,
        damage_old,
        crack_seeds,
        irreversible,
        line_inverses,
        change,
    )
    every = exchange(jnp.broadcast_to(change, (devices, 128)))
    global_sums = jnp.sum(every, axis=0)[:2]
    update_norms = jnp.sqrt(global_sums / cell_count + EPSILON) / STEP
    return (damage, update_norms)


def solution(mesh):
    finer = Mesh(mesh.devices.reshape(8, 2, 2, 4, 4), ALL)
    spec = P(COL, ROW, None)
    in_specs = (spec, spec, spec, spec, P(), P())
    return jax.shard_map(local, mesh=finer, in_specs=in_specs, out_specs=(spec, P()), check_vma=False)
```

```python
import jax
import jax.numpy as jnp
from jax import lax
from jax.experimental import pallas as pl
from jax.experimental.pallas import tpu as pltpu
from jax.sharding import Mesh
from jax.sharding import PartitionSpec as P

ROW = ("row_0", "row_1", "row_2")
COL = ("col_0", "col_1")
ALL = ROW + COL
PLANE = ROW[1:] + COL

ITERS = 2

KAPPA = 2.0
STEP = 0.02
COUPLE = 0.5
EPSILON = 1e-06
HALF = 64


def iota(shape, axis):
    return lax.broadcasted_iota(jnp.int32, shape, axis)


def lane_lap(field):
    extent = field.shape[1]
    lane = iota(field.shape, 1)
    ahead = jnp.where(lane == extent - 1, field, pltpu.roll(field, extent - 1, 1))
    behind = jnp.where(lane == 0, field, pltpu.roll(field, 1, 1))
    return (ahead - field) + (behind - field)


def plane_lap(field, planes):
    extent = field.shape[0]
    plane = iota(field.shape, 0) % planes
    ahead = jnp.where(plane == planes - 1, field, pltpu.roll(field, extent - 1, 0))
    behind = jnp.where(plane == 0, field, pltpu.roll(field, 1, 0))
    return (ahead - field) + (behind - field)


def line_solve(lines, inverses_ref):
    count = lines.shape[0]
    blocks, cells, _ = inverses_ref.shape
    unit_row = iota((8, cells), 0)
    unit_lane = iota((8, cells), 1)
    units = jnp.where(
        ((unit_row == 0) & (unit_lane == 0)) | ((unit_row == 1) & (unit_lane == cells - 1)), 1.0, 0.0
    )
    products, firsts, lasts = [], [], []
    for k in range(blocks):
        stacked = jnp.concatenate([lines[:, k * cells : (k + 1) * cells], units], axis=0)
        result = lax.dot_general(
            stacked,
            inverses_ref[k],
            (((1,), (1,)), ((), ())),
            precision=lax.Precision.HIGHEST,
            preferred_element_type=jnp.float32,
        )
        products.append(result[:count])
        firsts.append(result[count : count + 1])
        lasts.append(result[count + 1 : count + 2])
    inflow = [jnp.zeros((count, 1), jnp.float32)]
    heads = []
    for k in range(blocks):
        heads.append(products[k][:, 0:1] + COUPLE * inflow[k] * firsts[k][:, 0:1])
        if k < blocks - 1:
            inflow.append(
                products[k][:, cells - 1 : cells] + COUPLE * inflow[k] * firsts[k][:, cells - 1 : cells]
            )
    outflow = [None] * blocks
    carried = heads[blocks - 1]
    for k in range(blocks - 2, -1, -1):
        outflow[k] = carried
        carried = heads[k] + COUPLE * carried * lasts[k][:, 0:1]
    solved = []
    for k in range(blocks):
        value = products[k]
        if k > 0:
            value = value + (COUPLE * inflow[k]) * firsts[k]
        if k < blocks - 1:
            value = value + (COUPLE * outflow[k]) * lasts[k]
        solved.append(value)
    return jnp.concatenate(solved, axis=1)


def send_rows(out_ref, field, first, stride):
    chunks = field.shape[1] // 4
    for s in range(2):
        pair = jnp.concatenate(
            [field[:, 2 * s * chunks : (2 * s + 1) * chunks], field[:, (2 * s + 1) * chunks : (2 * s + 2) * chunks]],
            axis=0,
        )
        out_ref[pl.ds(first + s, chunks, stride=stride), :] = pair.T


def receive_rows(in_ref, first, stride):
    chunks = in_ref.shape[0] // stride
    parts = []
    for s in range(2):
        pair = in_ref[pl.ds(first + s, chunks, stride=stride), :].T
        parts.append(pair[:HALF])
        parts.append(pair[HALF:])
    return jnp.concatenate(parts, axis=1)


def gather_lines(in_ref, planes, first, stride):
    rows = in_ref.shape[0] // (stride * planes)
    low = iota((planes, 2 * HALF), 1) < HALF
    lines = [[], [], [], []]
    for j in range(rows // 2):
        for s in range(2):
            even = in_ref[pl.ds(2 * j * stride * planes + first + s, planes, stride=stride), :]
            odd = in_ref[pl.ds((2 * j + 1) * stride * planes + first + s, planes, stride=stride), :]
            lines[2 * s].append(jnp.where(low, even, pltpu.roll(odd, HALF, 1)))
            lines[2 * s + 1].append(jnp.where(low, pltpu.roll(even, HALF, 1), odd))
    return jnp.concatenate([jnp.concatenate(line, axis=1) for line in lines], axis=0)


def scatter_lines(out_ref, lines, planes, first, stride):
    rows = out_ref.shape[0] // (stride * planes)
    low = iota((planes, 2 * HALF), 1) < HALF
    for j in range(rows // 2):
        for s in range(2):
            one = lines[2 * s * planes : (2 * s + 1) * planes, j * 128 : (j + 1) * 128]
            two = lines[(2 * s + 1) * planes : (2 * s + 2) * planes, j * 128 : (j + 1) * 128]
            out_ref[pl.ds(2 * j * stride * planes + first + s, planes, stride=stride), :] = jnp.where(
                low, one, pltpu.roll(two, HALF, 1)
            )
            out_ref[pl.ds((2 * j + 1) * stride * planes + first + s, planes, stride=stride), :] = jnp.where(
                low, pltpu.roll(one, HALF, 1), two
            )


def plane_mix(z_inverse, lines):
    planes = z_inverse.shape[0]
    copies = lines.shape[0] // planes
    tiled = jnp.concatenate([jnp.concatenate([z_inverse] * copies, axis=1)] * copies, axis=0)
    same = iota(tiled.shape, 0) // planes == iota(tiled.shape, 1) // planes
    return jnp.dot(
        jnp.where(same, tiled, 0.0), lines, precision=lax.Precision.HIGHEST, preferred_element_type=jnp.float32
    )


def bound(old, seeds, irreversible):
    return jnp.where(seeds == 1, 1.0, jnp.where(irreversible == 1, old, 0.0))


def clamp(damage, update, lower_bound):
    return jnp.minimum(jnp.maximum(damage + update, lower_bound), 1.0)


def first_kernel(
    energy_hbm, old_hbm, seeds_hbm, irreversible_hbm, inverses_hbm,
    out_ref,
    energy_ref, old_ref, seeds_ref, irreversible_ref, inverses_ref, sems,
):
    pairs = [
        (old_hbm, old_ref), (seeds_hbm, seeds_ref), (energy_hbm, energy_ref),
        (inverses_hbm, inverses_ref), (irreversible_hbm, irreversible_ref),
    ]
    copies = [pltpu.make_async_copy(src, dst, sems.at[i]) for i, (src, dst) in enumerate(pairs)]
    for copy in copies:
        copy.start()
    copies[0].wait()
    copies[1].wait()
    damage = jnp.where(seeds_ref[0] == 1, 1.0, old_ref[0])
    send_rows(out_ref, damage, 4, 10)
    copies[2].wait()
    energy = energy_ref[0]
    send_rows(out_ref, energy, 8, 10)
    partial_value = energy - (1.0 + energy) * damage + KAPPA * lane_lap(damage)
    copies[3].wait()
    count = damage.shape[0]
    solved = line_solve(jnp.concatenate([partial_value, damage], axis=0), inverses_ref)
    send_rows(out_ref, solved[:count], 0, 10)
    send_rows(out_ref, solved[count:], 2, 10)
    copies[4].wait()
    send_rows(out_ref, bound(old_ref[0], seeds_ref[0], irreversible_ref[0]), 6, 10)


def cross_kernel(in_ref, inverses_ref, z_ref, out_ref, change_ref):
    z_inverse = z_ref[...]
    planes = z_inverse.shape[0]
    solved_damage = gather_lines(in_ref, planes, 2, 10)
    turned = gather_lines(in_ref, planes, 0, 10) + KAPPA * (
        lane_lap(solved_damage) + plane_lap(solved_damage, planes)
    )
    update = STEP * plane_mix(z_inverse, line_solve(turned, inverses_ref))
    damage = gather_lines(in_ref, planes, 4, 10)
    renewed = clamp(damage, update, gather_lines(in_ref, planes, 6, 10))
    change_ref[...] = jnp.full(change_ref.shape, jnp.sum((renewed - damage) ** 2), jnp.float32)
    scatter_lines(out_ref, renewed, planes, 4, 6)
    energy = gather_lines(in_ref, planes, 8, 10)
    partial_value = energy - (1.0 + energy) * renewed + KAPPA * (lane_lap(renewed) + plane_lap(renewed, planes))
    count = renewed.shape[0]
    solved = line_solve(jnp.concatenate([partial_value, renewed], axis=0), inverses_ref)
    scatter_lines(out_ref, plane_mix(z_inverse, solved[:count]), planes, 0, 6)
    scatter_lines(out_ref, plane_mix(z_inverse, solved[count:]), planes, 2, 6)


def last_kernel(
    in_ref, old_ref, seeds_ref, irreversible_ref, inverses_ref, first_change_ref, damage_ref, change_ref
):
    solved_part = receive_rows(in_ref, 0, 6)
    solved_damage = receive_rows(in_ref, 2, 6)
    update = STEP * line_solve(solved_part + KAPPA * lane_lap(solved_damage), inverses_ref)
    damage = receive_rows(in_ref, 4, 6)
    renewed = clamp(damage, update, bound(old_ref[0], seeds_ref[0], irreversible_ref[0]))
    damage_ref[0] = renewed
    change = jnp.sum((renewed - damage) ** 2)
    lane = iota(change_ref.shape, 1)
    change_ref[...] = jnp.where(lane == 0, first_change_ref[...], jnp.where(lane == 1, change, 0.0))


def call(kernel, outs, *args, direct=True, scratch=()):
    space = pltpu.VMEM if direct else pl.ANY
    if not direct:
        args = [pltpu.with_memory_space_constraint(arg, pltpu.HBM) for arg in args]
    return pl.pallas_call(
        kernel,
        out_shape=[jax.ShapeDtypeStruct(shape, jnp.float32) for shape in outs],
        in_specs=[pl.BlockSpec(memory_space=space) for _ in args],
        out_specs=[pl.BlockSpec(memory_space=pltpu.VMEM) for _ in outs],
        scratch_shapes=scratch,
        compiler_params=pltpu.CompilerParams(vmem_limit_bytes=20 * 1024 * 1024),
    )(*args)


def exchange(rows, axes):
    return lax.all_to_all(rows, axes, split_axis=0, concat_axis=0, tiled=True)


def cross(rows):
    pairs = rows.reshape(-1, 2, 128)
    return exchange(pairs, ALL).reshape(rows.shape)


def local(energy, damage_old, crack_seeds, irreversible, line_inverses, z_inverse):
    planes, rows_here, line_length = energy.shape
    cell_count = planes * rows_here * line_length * lax.axis_size(ALL)
    one = planes * rows_here * line_length // 128
    inputs = (energy, damage_old, crack_seeds, irreversible, line_inverses)
    scratch = [pltpu.VMEM(part.shape, part.dtype) for part in inputs] + [pltpu.SemaphoreType.DMA((5,))]
    (sent,) = call(first_kernel, [(5 * one, 128)], *inputs, direct=False, scratch=scratch)
    sent, change = call(cross_kernel, [(3 * one, 128), (1, 128)], cross(sent), line_inverses, z_inverse)
    damage, change = call(
        last_kernel,
        [energy.shape, (lax.axis_size(PLANE), 128)],
        cross(sent),
        damage_old,
        crack_seeds,
        irreversible,
        line_inverses,
        change,
    )
    plane_sums = jnp.sum(exchange(change, PLANE), axis=0, keepdims=True)
    every = exchange(jnp.broadcast_to(plane_sums, (lax.axis_size(ROW[0]), 128)), ROW[:1])
    global_sums = jnp.sum(every, axis=0)[:ITERS]
    update_norms = jnp.sqrt(global_sums / cell_count + EPSILON) / STEP
    return (damage, update_norms)


def solution(mesh):
    finer = Mesh(mesh.devices.reshape(8, 2, 2, 4, 4), ALL)
    spec = P(COL, ROW, None)
    in_specs = (spec, spec, spec, spec, P(), P())
    return jax.shard_map(local, mesh=finer, in_specs=in_specs, out_specs=(spec, P()), check_vma=False)
```

```python
import jax
import jax.numpy as jnp
from jax import lax
from jax.experimental import pallas as pl
from jax.experimental.pallas import tpu as pltpu
from jax.sharding import Mesh
from jax.sharding import PartitionSpec as P

ROW = ("row_0", "row_1", "row_2")
COL = ("col_0", "col_1")
ALL = ROW + COL
PLANE = ROW[1:] + COL

ITERS = 2

KAPPA = 2.0
STEP = 0.02
COUPLE = 0.5
EPSILON = 1e-06
HALF = 64


def iota(shape, axis):
    return lax.broadcasted_iota(jnp.int32, shape, axis)


def lane_lap(field):
    extent = field.shape[1]
    lane = iota(field.shape, 1)
    ahead = jnp.where(lane == extent - 1, field, pltpu.roll(field, extent - 1, 1))
    behind = jnp.where(lane == 0, field, pltpu.roll(field, 1, 1))
    return (ahead - field) + (behind - field)


def plane_lap(field, planes):
    extent = field.shape[0]
    plane = iota(field.shape, 0) % planes
    ahead = jnp.where(plane == planes - 1, field, pltpu.roll(field, extent - 1, 0))
    behind = jnp.where(plane == 0, field, pltpu.roll(field, 1, 0))
    return (ahead - field) + (behind - field)


def halves(value):
    high = value.astype(jnp.bfloat16)
    return high, (value - high.astype(jnp.float32)).astype(jnp.bfloat16)


def product(rows, high, low, dims):
    count = rows.shape[0]
    rows_high, rows_low = halves(rows)
    both = lax.dot_general(
        jnp.concatenate([rows_high, rows_low], axis=0), high, (dims, ((), ())), preferred_element_type=jnp.float32
    )
    rest = lax.dot_general(rows_high, low, (dims, ((), ())), preferred_element_type=jnp.float32)
    return both[:count] + both[count:] + rest


def split_inverses(inverses_ref, high_ref, low_ref, ends_ref):
    blocks, cells, _ = inverses_ref.shape
    unit_row = iota((16, cells), 0)
    unit_lane = iota((16, cells), 1)
    units = jnp.where(
        ((unit_row == 0) & (unit_lane == 0)) | ((unit_row == 1) & (unit_lane == cells - 1)), 1.0, 0.0
    ).astype(jnp.bfloat16)
    for k in range(blocks):
        high, low = halves(inverses_ref[k])
        high_ref[k] = high
        low_ref[k] = low
        dims = (((1,), (1,)), ((), ()))
        ends = lax.dot_general(units, high, dims, preferred_element_type=jnp.float32) + lax.dot_general(
            units, low, dims, preferred_element_type=jnp.float32
        )
        ends_ref[k] = ends[:8]


def line_solve(lines, high_ref, low_ref, ends_ref):
    count = lines.shape[0]
    blocks, cells, _ = high_ref.shape
    products, firsts, lasts = [], [], []
    for k in range(blocks):
        products.append(product(lines[:, k * cells : (k + 1) * cells], high_ref[k], low_ref[k], ((1,), (1,))))
        firsts.append(ends_ref[k, 0:1, :])
        lasts.append(ends_ref[k, 1:2, :])
    inflow = [jnp.zeros((count, 1), jnp.float32)]
    heads = []
    for k in range(blocks):
        heads.append(products[k][:, 0:1] + COUPLE * inflow[k] * firsts[k][:, 0:1])
        if k < blocks - 1:
            inflow.append(
                products[k][:, cells - 1 : cells] + COUPLE * inflow[k] * firsts[k][:, cells - 1 : cells]
            )
    outflow = [None] * blocks
    carried = heads[blocks - 1]
    for k in range(blocks - 2, -1, -1):
        outflow[k] = carried
        carried = heads[k] + COUPLE * carried * lasts[k][:, 0:1]
    solved = []
    for k in range(blocks):
        value = products[k]
        if k > 0:
            value = value + (COUPLE * inflow[k]) * firsts[k]
        if k < blocks - 1:
            value = value + (COUPLE * outflow[k]) * lasts[k]
        solved.append(value)
    return jnp.concatenate(solved, axis=1)


def send_rows(out_ref, field, first, stride):
    chunks = field.shape[1] // 4
    for s in range(2):
        pair = jnp.concatenate(
            [field[:, 2 * s * chunks : (2 * s + 1) * chunks], field[:, (2 * s + 1) * chunks : (2 * s + 2) * chunks]],
            axis=0,
        )
        out_ref[pl.ds(first + s, chunks, stride=stride), :] = pair.T


def receive_rows(in_ref, first, stride):
    chunks = in_ref.shape[0] // stride
    parts = []
    for s in range(2):
        pair = in_ref[pl.ds(first + s, chunks, stride=stride), :].T
        parts.append(pair[:HALF])
        parts.append(pair[HALF:])
    return jnp.concatenate(parts, axis=1)


def gather_lines(in_ref, planes, first, stride):
    rows = in_ref.shape[0] // (stride * planes)
    low = iota((planes, 2 * HALF), 1) < HALF
    lines = [[], [], [], []]
    for j in range(rows // 2):
        for s in range(2):
            even = in_ref[pl.ds(2 * j * stride * planes + first + s, planes, stride=stride), :]
            odd = in_ref[pl.ds((2 * j + 1) * stride * planes + first + s, planes, stride=stride), :]
            lines[2 * s].append(jnp.where(low, even, pltpu.roll(odd, HALF, 1)))
            lines[2 * s + 1].append(jnp.where(low, pltpu.roll(even, HALF, 1), odd))
    return jnp.concatenate([jnp.concatenate(line, axis=1) for line in lines], axis=0)


def scatter_lines(out_ref, lines, planes, first, stride):
    rows = out_ref.shape[0] // (stride * planes)
    low = iota((planes, 2 * HALF), 1) < HALF
    for j in range(rows // 2):
        for s in range(2):
            one = lines[2 * s * planes : (2 * s + 1) * planes, j * 128 : (j + 1) * 128]
            two = lines[(2 * s + 1) * planes : (2 * s + 2) * planes, j * 128 : (j + 1) * 128]
            out_ref[pl.ds(2 * j * stride * planes + first + s, planes, stride=stride), :] = jnp.where(
                low, one, pltpu.roll(two, HALF, 1)
            )
            out_ref[pl.ds((2 * j + 1) * stride * planes + first + s, planes, stride=stride), :] = jnp.where(
                low, pltpu.roll(one, HALF, 1), two
            )


def plane_mix(z_inverse, lines):
    planes = z_inverse.shape[0]
    copies = lines.shape[0] // planes
    tiled = jnp.concatenate([jnp.concatenate([z_inverse] * copies, axis=1)] * copies, axis=0)
    same = iota(tiled.shape, 0) // planes == iota(tiled.shape, 1) // planes
    high, low = halves(lines)
    return product(jnp.where(same, tiled, 0.0), high, low, ((1,), (0,)))


def bound(old, seeds, irreversible):
    return jnp.where(seeds == 1, 1.0, jnp.where(irreversible == 1, old, 0.0))


def clamp(damage, update, lower_bound):
    return jnp.minimum(jnp.maximum(damage + update, lower_bound), 1.0)


def first_kernel(
    energy_hbm, old_hbm, seeds_hbm, irreversible_hbm, inverses_hbm,
    out_ref, high_ref, low_ref, ends_ref,
    energy_ref, old_ref, seeds_ref, irreversible_ref, inverses_ref, sems,
):
    pairs = [
        (old_hbm, old_ref), (seeds_hbm, seeds_ref), (energy_hbm, energy_ref),
        (inverses_hbm, inverses_ref), (irreversible_hbm, irreversible_ref),
    ]
    copies = [pltpu.make_async_copy(src, dst, sems.at[i]) for i, (src, dst) in enumerate(pairs)]
    for copy in copies:
        copy.start()
    copies[0].wait()
    copies[1].wait()
    damage = jnp.where(seeds_ref[0] == 1, 1.0, old_ref[0])
    send_rows(out_ref, damage, 4, 10)
    copies[2].wait()
    energy = energy_ref[0]
    send_rows(out_ref, energy, 8, 10)
    partial_value = energy - (1.0 + energy) * damage + KAPPA * lane_lap(damage)
    copies[3].wait()
    split_inverses(inverses_ref, high_ref, low_ref, ends_ref)
    count = damage.shape[0]
    solved = line_solve(jnp.concatenate([partial_value, damage], axis=0), high_ref, low_ref, ends_ref)
    send_rows(out_ref, solved[:count], 0, 10)
    send_rows(out_ref, solved[count:], 2, 10)
    copies[4].wait()
    send_rows(out_ref, bound(old_ref[0], seeds_ref[0], irreversible_ref[0]), 6, 10)


def cross_kernel(in_ref, high_ref, low_ref, ends_ref, z_ref, out_ref, change_ref):
    z_inverse = z_ref[...]
    planes = z_inverse.shape[0]
    solved_damage = gather_lines(in_ref, planes, 2, 10)
    turned = gather_lines(in_ref, planes, 0, 10) + KAPPA * (
        lane_lap(solved_damage) + plane_lap(solved_damage, planes)
    )
    update = STEP * plane_mix(z_inverse, line_solve(turned, high_ref, low_ref, ends_ref))
    damage = gather_lines(in_ref, planes, 4, 10)
    renewed = clamp(damage, update, gather_lines(in_ref, planes, 6, 10))
    change_ref[...] = jnp.full(change_ref.shape, jnp.sum((renewed - damage) ** 2), jnp.float32)
    scatter_lines(out_ref, renewed, planes, 4, 6)
    energy = gather_lines(in_ref, planes, 8, 10)
    partial_value = energy - (1.0 + energy) * renewed + KAPPA * (lane_lap(renewed) + plane_lap(renewed, planes))
    count = renewed.shape[0]
    solved = line_solve(jnp.concatenate([partial_value, renewed], axis=0), high_ref, low_ref, ends_ref)
    scatter_lines(out_ref, plane_mix(z_inverse, solved[:count]), planes, 0, 6)
    scatter_lines(out_ref, plane_mix(z_inverse, solved[count:]), planes, 2, 6)


def last_kernel(
    in_ref, old_ref, seeds_ref, irreversible_ref, high_ref, low_ref, ends_ref, first_change_ref, damage_ref, change_ref
):
    solved_part = receive_rows(in_ref, 0, 6)
    solved_damage = receive_rows(in_ref, 2, 6)
    turned = solved_part + KAPPA * lane_lap(solved_damage)
    update = STEP * line_solve(turned, high_ref, low_ref, ends_ref)
    damage = receive_rows(in_ref, 4, 6)
    renewed = clamp(damage, update, bound(old_ref[0], seeds_ref[0], irreversible_ref[0]))
    damage_ref[0] = renewed
    change = jnp.sum((renewed - damage) ** 2)
    lane = iota(change_ref.shape, 1)
    change_ref[...] = jnp.where(lane == 0, first_change_ref[...], jnp.where(lane == 1, change, 0.0))


def call(kernel, outs, *args, direct=True, scratch=()):
    space = pltpu.VMEM if direct else pl.ANY
    if not direct:
        args = [pltpu.with_memory_space_constraint(arg, pltpu.HBM) for arg in args]
    return pl.pallas_call(
        kernel,
        out_shape=[jax.ShapeDtypeStruct(shape, dtype) for shape, dtype in outs],
        in_specs=[pl.BlockSpec(memory_space=space) for _ in args],
        out_specs=[pl.BlockSpec(memory_space=pltpu.VMEM) for _ in outs],
        scratch_shapes=scratch,
        compiler_params=pltpu.CompilerParams(vmem_limit_bytes=20 * 1024 * 1024),
    )(*args)


def exchange(rows, axes):
    return lax.all_to_all(rows, axes, split_axis=0, concat_axis=0, tiled=True)


def cross(rows):
    pairs = rows.reshape(-1, 2, 128)
    return exchange(pairs, ALL).reshape(rows.shape)


def local(energy, damage_old, crack_seeds, irreversible, line_inverses, z_inverse):
    planes, rows_here, line_length = energy.shape
    cell_count = planes * rows_here * line_length * lax.axis_size(ALL)
    one = planes * rows_here * line_length // 128
    inputs = (energy, damage_old, crack_seeds, irreversible, line_inverses)
    scratch = [pltpu.VMEM(part.shape, part.dtype) for part in inputs] + [pltpu.SemaphoreType.DMA((5,))]
    f32, bf16 = jnp.float32, jnp.bfloat16
    blocks, cells, _ = line_inverses.shape
    sent, *split = call(
        first_kernel,
        [((5 * one, 128), f32), (line_inverses.shape, bf16), (line_inverses.shape, bf16), ((blocks, 8, cells), f32)],
        *inputs,
        direct=False,
        scratch=scratch,
    )
    sent, change = call(
        cross_kernel, [((3 * one, 128), f32), ((1, 128), f32)], cross(sent), *split, z_inverse
    )
    damage, change = call(
        last_kernel,
        [(energy.shape, f32), ((lax.axis_size(PLANE), 128), f32)],
        cross(sent),
        damage_old,
        crack_seeds,
        irreversible,
        *split,
        change,
    )
    plane_sums = jnp.sum(exchange(change, PLANE), axis=0, keepdims=True)
    every = exchange(jnp.broadcast_to(plane_sums, (lax.axis_size(ROW[0]), 128)), ROW[:1])
    global_sums = jnp.sum(every, axis=0)[:ITERS]
    update_norms = jnp.sqrt(global_sums / cell_count + EPSILON) / STEP
    return (damage, update_norms)


def solution(mesh):
    finer = Mesh(mesh.devices.reshape(8, 2, 2, 4, 4), ALL)
    spec = P(COL, ROW, None)
    in_specs = (spec, spec, spec, spec, P(), P())
    return jax.shard_map(local, mesh=finer, in_specs=in_specs, out_specs=(spec, P()), check_vma=False)
```

```python
import jax
import jax.numpy as jnp
from jax import lax
from jax.experimental import pallas as pl
from jax.experimental.pallas import tpu as pltpu
from jax.sharding import Mesh
from jax.sharding import PartitionSpec as P

ROW = ("row_0", "row_1", "row_2")
COL = ("col_0", "col_1")
ALL = ROW + COL
PLANE = ROW[1:] + COL

ITERS = 2

KAPPA = 2.0
STEP = 0.02
COUPLE = 0.5
EPSILON = 1e-06
HALF = 64


def iota(shape, axis):
    return lax.broadcasted_iota(jnp.int32, shape, axis)


def lane_lap(field):
    extent = field.shape[1]
    lane = iota(field.shape, 1)
    ahead = jnp.where(lane == extent - 1, field, pltpu.roll(field, extent - 1, 1))
    behind = jnp.where(lane == 0, field, pltpu.roll(field, 1, 1))
    return (ahead - field) + (behind - field)


def plane_lap(field, planes):
    extent = field.shape[0]
    plane = iota(field.shape, 0) % planes
    ahead = jnp.where(plane == planes - 1, field, pltpu.roll(field, extent - 1, 0))
    behind = jnp.where(plane == 0, field, pltpu.roll(field, 1, 0))
    return (ahead - field) + (behind - field)


def halves(value):
    high = value.astype(jnp.bfloat16)
    return high, (value - high.astype(jnp.float32)).astype(jnp.bfloat16)


def product(rows, high, low, dims):
    count = rows.shape[0]
    rows_high, rows_low = halves(rows)
    both = lax.dot_general(
        jnp.concatenate([rows_high, rows_low], axis=0), high, (dims, ((), ())), preferred_element_type=jnp.float32
    )
    rest = lax.dot_general(rows_high, low, (dims, ((), ())), preferred_element_type=jnp.float32)
    return both[:count] + both[count:] + rest


def split_inverses(inverses_ref, high_ref, low_ref, ends_ref):
    blocks, cells, _ = inverses_ref.shape
    unit_row = iota((16, cells), 0)
    unit_lane = iota((16, cells), 1)
    units = jnp.where(
        ((unit_row == 0) & (unit_lane == 0)) | ((unit_row == 1) & (unit_lane == cells - 1)), 1.0, 0.0
    ).astype(jnp.bfloat16)
    for k in range(blocks):
        high, low = halves(inverses_ref[k])
        high_ref[k] = high
        low_ref[k] = low
        dims = (((1,), (1,)), ((), ()))
        ends = lax.dot_general(units, high, dims, preferred_element_type=jnp.float32) + lax.dot_general(
            units, low, dims, preferred_element_type=jnp.float32
        )
        ends_ref[k] = ends[:8]
        ends_ref[k, 2:3, :] = jnp.broadcast_to(ends[0:1, 0:1], (1, cells))
        ends_ref[k, 3:4, :] = jnp.broadcast_to(ends[0:1, cells - 1 : cells], (1, cells))
        ends_ref[k, 4:5, :] = jnp.broadcast_to(ends[1:2, 0:1], (1, cells))


def line_solve(lines, high_ref, low_ref, ends_ref):
    count = lines.shape[0]
    blocks, cells, _ = high_ref.shape
    products, firsts, lasts = [], [], []
    for k in range(blocks):
        products.append(product(lines[:, k * cells : (k + 1) * cells], high_ref[k], low_ref[k], ((1,), (1,))))
        firsts.append(ends_ref[k, 0:1, :])
        lasts.append(ends_ref[k, 1:2, :])
    wide = (count, 128)
    inflow, outflow = [None], [None] * blocks
    heads = [jnp.broadcast_to(products[0][:, 0:1], wide)]
    carried = jnp.broadcast_to(products[0][:, cells - 1 : cells], wide)
    for k in range(1, blocks):
        inflow.append(COUPLE * carried)
        heads.append(jnp.broadcast_to(products[k][:, 0:1], wide) + inflow[k] * ends_ref[k, 2:3, :128])
        if k < blocks - 1:
            carried = (
                jnp.broadcast_to(products[k][:, cells - 1 : cells], wide) + inflow[k] * ends_ref[k, 3:4, :128]
            )
    carried = heads[blocks - 1]
    for k in range(blocks - 2, -1, -1):
        outflow[k] = COUPLE * carried
        carried = heads[k] + outflow[k] * ends_ref[k, 4:5, :128]
    solved = []
    for k in range(blocks):
        for half in range(0, cells, 128):
            value = products[k][:, half : half + 128]
            if k > 0:
                value = value + inflow[k] * firsts[k][:, half : half + 128]
            if k < blocks - 1:
                value = value + outflow[k] * lasts[k][:, half : half + 128]
            solved.append(value)
    return jnp.concatenate(solved, axis=1)


def low_half(count):
    return iota((count, 2 * HALF), 1) < HALF


def send_pair(out_ref, flat_ref, stacked, first, stride):
    chunks = out_ref.shape[0] // stride
    for t in range(0, 4 * chunks, 128):
        flat_ref[t : t + 128, :] = stacked[:, t : t + 128].T
    for i in range(4):
        out_ref[pl.ds(first + i, chunks, stride=stride), :] = flat_ref[pl.ds(i, chunks, stride=4), :]


def send_single(out_ref, flat_ref, field, first, stride):
    chunks = out_ref.shape[0] // stride
    doubled = jnp.concatenate([field, field], axis=0)
    for t in range(0, 4 * chunks, 128):
        flat_ref[t : t + 128, :] = doubled[:, t : t + 128].T
    for i in range(2):
        out_ref[pl.ds(first + i, chunks, stride=stride), :] = jnp.where(
            low_half(chunks),
            flat_ref[pl.ds(i, chunks, stride=4), :],
            flat_ref[pl.ds(i + 2, chunks, stride=4), :],
        )


def gather_row(in_ref, planes, at, stride):
    rows = in_ref.shape[0] // (stride * planes)
    low = low_half(planes)
    ones, twos = [], []
    for j in range(rows // 2):
        even = in_ref[pl.ds(2 * j * stride * planes + at, planes, stride=stride), :]
        odd = in_ref[pl.ds((2 * j + 1) * stride * planes + at, planes, stride=stride), :]
        ones.append(jnp.where(low, even, pltpu.roll(odd, HALF, 1)))
        twos.append(jnp.where(low, pltpu.roll(even, HALF, 1), odd))
    return jnp.concatenate(ones, axis=1), jnp.concatenate(twos, axis=1)


def scatter_row(out_ref, ones, twos, planes, at, stride):
    rows = out_ref.shape[0] // (stride * planes)
    low = low_half(planes)
    for j in range(rows // 2):
        one = ones[:, j * 128 : (j + 1) * 128]
        two = twos[:, j * 128 : (j + 1) * 128]
        out_ref[pl.ds(2 * j * stride * planes + at, planes, stride=stride), :] = jnp.where(
            low, one, pltpu.roll(two, HALF, 1)
        )
        out_ref[pl.ds((2 * j + 1) * stride * planes + at, planes, stride=stride), :] = jnp.where(
            low, pltpu.roll(one, HALF, 1), two
        )


def gather_pair(in_ref, planes, first, stride):
    pairs = [gather_row(in_ref, planes, first + i, stride) for i in range(4)]
    return [jnp.concatenate(part, axis=0) for part in zip(*pairs)]


def gather_single(in_ref, planes, first, stride):
    pairs = [gather_row(in_ref, planes, first + i, stride) for i in range(2)]
    return jnp.concatenate([part[half] for half in range(2) for part in pairs], axis=0)


def plane_mix(z_inverse, lines):
    planes = z_inverse.shape[0]
    copies = lines.shape[0] // planes
    tiled = jnp.concatenate([jnp.concatenate([z_inverse] * copies, axis=1)] * copies, axis=0)
    same = iota(tiled.shape, 0) // planes == iota(tiled.shape, 1) // planes
    high, low = halves(lines)
    return product(jnp.where(same, tiled, 0.0), high, low, ((1,), (0,)))


def bound(old, seeds, irreversible):
    return jnp.where(seeds == 1, 1.0, jnp.where(irreversible == 1, old, 0.0))


def clamp(damage, update, lower_bound):
    return jnp.minimum(jnp.maximum(damage + update, lower_bound), 1.0)


def first_kernel(
    energy_hbm, old_hbm, seeds_hbm, irreversible_hbm, inverses_hbm,
    out_ref, high_ref, low_ref, ends_ref,
    energy_ref, old_ref, seeds_ref, irreversible_ref, inverses_ref, flat_refs, sems,
):
    pairs = [
        (inverses_hbm, inverses_ref), (old_hbm, old_ref), (seeds_hbm, seeds_ref),
        (energy_hbm, energy_ref), (irreversible_hbm, irreversible_ref),
    ]
    copies = [pltpu.make_async_copy(src, dst, sems.at[i]) for i, (src, dst) in enumerate(pairs)]
    for copy in copies:
        copy.start()
    copies[0].wait()
    split_inverses(inverses_ref, high_ref, low_ref, ends_ref)
    for copy in copies[1:]:
        copy.wait()
    damage = jnp.where(seeds_ref[0] == 1, 1.0, old_ref[0])
    energy = energy_ref[0]
    partial_value = energy - (1.0 + energy) * damage + KAPPA * lane_lap(damage)
    solved = line_solve(jnp.concatenate([partial_value, damage], axis=0), high_ref, low_ref, ends_ref)
    lower = bound(old_ref[0], seeds_ref[0], irreversible_ref[0])
    send_pair(out_ref, flat_refs.at[0], jnp.concatenate([damage, lower], axis=0), 4, 10)
    send_single(out_ref, flat_refs.at[1], energy, 8, 10)
    send_pair(out_ref, flat_refs.at[2], solved, 0, 10)


def cross_kernel(in_ref, high_ref, low_ref, ends_ref, z_ref, out_ref, change_ref):
    z_inverse = z_ref[...]
    planes = z_inverse.shape[0]
    solved_part, solved_damage = gather_pair(in_ref, planes, 0, 10)
    turned = solved_part + KAPPA * (lane_lap(solved_damage) + plane_lap(solved_damage, planes))
    update = STEP * plane_mix(z_inverse, line_solve(turned, high_ref, low_ref, ends_ref))
    damage, lower = gather_pair(in_ref, planes, 4, 10)
    renewed = clamp(damage, update, lower)
    change_ref[...] = jnp.full(change_ref.shape, jnp.sum((renewed - damage) ** 2), jnp.float32)
    energy = gather_single(in_ref, planes, 8, 10)
    partial_value = energy - (1.0 + energy) * renewed + KAPPA * (lane_lap(renewed) + plane_lap(renewed, planes))
    count = renewed.shape[0]
    solved = line_solve(jnp.concatenate([partial_value, renewed], axis=0), high_ref, low_ref, ends_ref)
    solved_part = plane_mix(z_inverse, solved[:count])
    solved_damage = plane_mix(z_inverse, solved[count:])
    steps = KAPPA * (solved_damage[planes:] - solved_damage[:-planes])
    rim = jnp.zeros((planes, solved.shape[1]), jnp.float32)
    solved_part = solved_part + jnp.concatenate([steps, rim], axis=0) - jnp.concatenate([rim, steps], axis=0)
    for i in range(4):
        part = slice(i * planes, (i + 1) * planes)
        scatter_row(out_ref, solved_part[part], renewed[part], planes, i, 5)
    scatter_row(out_ref, solved_damage[:planes], solved_damage[-planes:], planes, 4, 5)


def last_kernel(
    in_ref, old_ref, seeds_ref, irreversible_ref, high_ref, low_ref, ends_ref, first_change_ref,
    damage_ref, change_ref,
    flat_ref,
):
    chunks = in_ref.shape[0] // 5
    edges = in_ref[pl.ds(4, chunks, stride=5), :]
    inner = low_half(chunks) & (iota((chunks, 128), 0) < chunks - 1)
    steps = pltpu.roll(edges, chunks - 1, 0) - pltpu.roll(edges, HALF, 1)
    steps = jnp.where(inner, KAPPA * steps, 0.0)
    for i in range(4):
        value = in_ref[pl.ds(i, chunks, stride=5), :]
        if i == 0:
            value = value - pltpu.roll(steps, 1, 0)
        if i == 3:
            value = value + steps
        flat_ref[pl.ds(i, chunks, stride=4), :] = value
    tiles = [flat_ref[t : t + 128, :].T for t in range(0, 4 * chunks, 128)]
    turned = jnp.concatenate([tile[:HALF] for tile in tiles], axis=1)
    damage = jnp.concatenate([tile[HALF:] for tile in tiles], axis=1)
    update = STEP * line_solve(turned, high_ref, low_ref, ends_ref)
    renewed = clamp(damage, update, bound(old_ref[0], seeds_ref[0], irreversible_ref[0]))
    damage_ref[0] = renewed
    change = jnp.sum((renewed - damage) ** 2)
    lane = iota(change_ref.shape, 1)
    change_ref[...] = jnp.where(lane == 0, first_change_ref[...], jnp.where(lane == 1, change, 0.0))


def call(kernel, outs, *args, direct=True, scratch=()):
    space = pltpu.VMEM if direct else pl.ANY
    if not direct:
        args = [pltpu.with_memory_space_constraint(arg, pltpu.HBM) for arg in args]
    return pl.pallas_call(
        kernel,
        out_shape=[jax.ShapeDtypeStruct(shape, dtype) for shape, dtype in outs],
        in_specs=[pl.BlockSpec(memory_space=space) for _ in args],
        out_specs=[pl.BlockSpec(memory_space=pltpu.VMEM) for _ in outs],
        scratch_shapes=scratch,
        compiler_params=pltpu.CompilerParams(vmem_limit_bytes=20 * 1024 * 1024),
    )(*args)


def exchange(rows, axes):
    return lax.all_to_all(rows, axes, split_axis=0, concat_axis=0, tiled=True)


def cross(rows):
    return exchange(rows.reshape(-1, 1, 128), ALL).reshape(rows.shape)


def local(energy, damage_old, crack_seeds, irreversible, line_inverses, z_inverse):
    planes, rows_here, line_length = energy.shape
    cell_count = planes * rows_here * line_length * lax.axis_size(ALL)
    one = planes * rows_here * line_length // 128
    inputs = (energy, damage_old, crack_seeds, irreversible, line_inverses)
    scratch = [pltpu.VMEM(part.shape, part.dtype) for part in inputs]
    scratch += [pltpu.VMEM((3, 2 * one, 128), jnp.float32), pltpu.SemaphoreType.DMA((5,))]
    f32, bf16 = jnp.float32, jnp.bfloat16
    blocks, cells, _ = line_inverses.shape
    sent, *split = call(
        first_kernel,
        [((5 * one, 128), f32), (line_inverses.shape, bf16), (line_inverses.shape, bf16), ((blocks, 8, cells), f32)],
        *inputs,
        direct=False,
        scratch=scratch,
    )
    sent, change = call(
        cross_kernel, [((5 * one // 2, 128), f32), ((1, 128), f32)], cross(sent), *split, z_inverse
    )
    damage, change = call(
        last_kernel,
        [(energy.shape, f32), ((lax.axis_size(PLANE), 128), f32)],
        cross(sent),
        damage_old,
        crack_seeds,
        irreversible,
        *split,
        change,
        scratch=[pltpu.VMEM((2 * one, 128), f32)],
    )
    plane_sums = jnp.sum(exchange(change, PLANE), axis=0, keepdims=True)
    every = exchange(jnp.broadcast_to(plane_sums, (lax.axis_size(ROW[0]), 128)), ROW[:1])
    global_sums = jnp.sum(every, axis=0)[:ITERS]
    update_norms = jnp.sqrt(global_sums / cell_count + EPSILON) / STEP
    return (damage, update_norms)


def solution(mesh):
    finer = Mesh(mesh.devices.reshape(8, 2, 2, 4, 4), ALL)
    spec = P(COL, ROW, None)
    in_specs = (spec, spec, spec, spec, P(), P())
    return jax.shard_map(local, mesh=finer, in_specs=in_specs, out_specs=(spec, P()), check_vma=False)
```

```python
import jax
import jax.numpy as jnp
from jax import lax
from jax.experimental import pallas as pl
from jax.experimental.pallas import tpu as pltpu
from jax.sharding import Mesh
from jax.sharding import PartitionSpec as P

ROW = ("row_0", "row_1", "row_2")
COL = ("col_0", "col_1")
ALL = ROW + COL
PLANE = ROW[1:] + COL

ITERS = 2

KAPPA = 2.0
STEP = 0.02
COUPLE = 0.5
EPSILON = 1e-06
HALF = 64


def iota(shape, axis):
    return lax.broadcasted_iota(jnp.int32, shape, axis)


def lane_lap(field):
    extent = field.shape[1]
    lane = iota(field.shape, 1)
    ahead = jnp.where(lane == extent - 1, field, pltpu.roll(field, extent - 1, 1))
    behind = jnp.where(lane == 0, field, pltpu.roll(field, 1, 1))
    return (ahead - field) + (behind - field)


def plane_lap(field, planes):
    extent = field.shape[0]
    plane = iota(field.shape, 0) % planes
    ahead = jnp.where(plane == planes - 1, field, pltpu.roll(field, extent - 1, 0))
    behind = jnp.where(plane == 0, field, pltpu.roll(field, 1, 0))
    return (ahead - field) + (behind - field)


def halves(value):
    high = value.astype(jnp.bfloat16)
    return high, (value - high.astype(jnp.float32)).astype(jnp.bfloat16)


def product(rows, high, low, dims):
    count = rows.shape[0]
    rows_high, rows_low = halves(rows)
    both = lax.dot_general(
        jnp.concatenate([rows_high, rows_low], axis=0), high, (dims, ((), ())), preferred_element_type=jnp.float32
    )
    rest = lax.dot_general(rows_high, low, (dims, ((), ())), preferred_element_type=jnp.float32)
    return both[:count] + both[count:] + rest


def split_inverses(inverses_ref, high_ref, low_ref, ends_ref):
    blocks, cells, _ = inverses_ref.shape
    unit_row = iota((16, cells), 0)
    unit_lane = iota((16, cells), 1)
    units = jnp.where(
        ((unit_row == 0) & (unit_lane == 0)) | ((unit_row == 1) & (unit_lane == cells - 1)), 1.0, 0.0
    ).astype(jnp.bfloat16)
    for k in range(blocks):
        high, low = halves(inverses_ref[k])
        high_ref[k] = high
        low_ref[k] = low
        dims = (((1,), (1,)), ((), ()))
        ends = lax.dot_general(units, high, dims, preferred_element_type=jnp.float32) + lax.dot_general(
            units, low, dims, preferred_element_type=jnp.float32
        )
        ends_ref[k] = ends[:8]
        ends_ref[k, 2:3, :] = jnp.broadcast_to(ends[0:1, 0:1], (1, cells))
        ends_ref[k, 3:4, :] = jnp.broadcast_to(ends[0:1, cells - 1 : cells], (1, cells))
        ends_ref[k, 4:5, :] = jnp.broadcast_to(ends[1:2, 0:1], (1, cells))


def line_solve(lines, high_ref, low_ref, ends_ref):
    count = lines.shape[0]
    blocks, cells, _ = high_ref.shape
    products, firsts, lasts = [], [], []
    for k in range(blocks):
        products.append(product(lines[:, k * cells : (k + 1) * cells], high_ref[k], low_ref[k], ((1,), (1,))))
        firsts.append(ends_ref[k, 0:1, :])
        lasts.append(ends_ref[k, 1:2, :])
    wide = (count, 128)
    inflow, outflow = [None], [None] * blocks
    heads = [jnp.broadcast_to(products[0][:, 0:1], wide)]
    carried = jnp.broadcast_to(products[0][:, cells - 1 : cells], wide)
    for k in range(1, blocks):
        inflow.append(COUPLE * carried)
        heads.append(jnp.broadcast_to(products[k][:, 0:1], wide) + inflow[k] * ends_ref[k, 2:3, :128])
        if k < blocks - 1:
            carried = (
                jnp.broadcast_to(products[k][:, cells - 1 : cells], wide) + inflow[k] * ends_ref[k, 3:4, :128]
            )
    carried = heads[blocks - 1]
    for k in range(blocks - 2, -1, -1):
        outflow[k] = COUPLE * carried
        carried = heads[k] + outflow[k] * ends_ref[k, 4:5, :128]
    solved = []
    for k in range(blocks):
        for half in range(0, cells, 128):
            value = products[k][:, half : half + 128]
            if k > 0:
                value = value + inflow[k] * firsts[k][:, half : half + 128]
            if k < blocks - 1:
                value = value + outflow[k] * lasts[k][:, half : half + 128]
            solved.append(value)
    return jnp.concatenate(solved, axis=1)


def low_half(count):
    return iota((count, 2 * HALF), 1) < HALF


def odd_rows():
    return lax.axis_index(ROW[-1]) == 1


def swap(odd, one, two):
    return jnp.where(odd, two, one), jnp.where(odd, one, two)


def send_pair(out_ref, flat_ref, stacked, first, stride):
    chunks = out_ref.shape[0] // stride
    for t in range(0, 4 * chunks, 128):
        flat_ref[t : t + 128, :] = stacked[:, t : t + 128].T
    for i in range(4):
        out_ref[pl.ds(first + i, chunks, stride=stride), :] = flat_ref[pl.ds(i, chunks, stride=4), :]


def send_single(out_ref, flat_ref, field, first, stride):
    chunks = out_ref.shape[0] // stride
    doubled = jnp.concatenate([field, field], axis=0)
    for t in range(0, 4 * chunks, 128):
        flat_ref[t : t + 128, :] = doubled[:, t : t + 128].T
    for i in range(2):
        out_ref[pl.ds(first + i, chunks, stride=stride), :] = jnp.where(
            low_half(chunks) != odd_rows(),
            flat_ref[pl.ds(i, chunks, stride=4), :],
            flat_ref[pl.ds(i + 2, chunks, stride=4), :],
        )


def gather_row(in_ref, planes, at, stride):
    rows = in_ref.shape[0] // (stride * planes)
    low = low_half(planes)
    ones, twos = [], []
    for j in range(rows // 2):
        even = in_ref[pl.ds(2 * j * stride * planes + at, planes, stride=stride), :]
        odd = in_ref[pl.ds((2 * j + 1) * stride * planes + at, planes, stride=stride), :]
        ones.append(jnp.where(low, even, odd))
        twos.append(pltpu.roll(jnp.where(low, odd, even), HALF, 1))
    return jnp.concatenate(ones, axis=1), jnp.concatenate(twos, axis=1)


def scatter_row(out_ref, ones, twos, planes, at, stride):
    rows = out_ref.shape[0] // (stride * planes)
    low = low_half(planes)
    for j in range(rows // 2):
        one = ones[:, j * 128 : (j + 1) * 128]
        two = pltpu.roll(twos[:, j * 128 : (j + 1) * 128], HALF, 1)
        out_ref[pl.ds(2 * j * stride * planes + at, planes, stride=stride), :] = jnp.where(
            low, one, two
        )
        out_ref[pl.ds((2 * j + 1) * stride * planes + at, planes, stride=stride), :] = jnp.where(
            low, two, one
        )


def gather_pair(in_ref, planes, first, stride):
    pairs = [gather_row(in_ref, planes, first + i, stride) for i in range(4)]
    return [jnp.concatenate(part, axis=0) for part in zip(*pairs)]


def gather_single(in_ref, planes, first, stride):
    pairs = [gather_row(in_ref, planes, first + i, stride) for i in range(2)]
    return jnp.concatenate([part[half] for half in range(2) for part in pairs], axis=0)


def plane_mix(z_inverse, lines):
    planes = z_inverse.shape[0]
    copies = lines.shape[0] // planes
    tiled = jnp.concatenate([jnp.concatenate([z_inverse] * copies, axis=1)] * copies, axis=0)
    same = iota(tiled.shape, 0) // planes == iota(tiled.shape, 1) // planes
    high, low = halves(lines)
    return product(jnp.where(same, tiled, 0.0), high, low, ((1,), (0,)))


def bound(old, seeds, irreversible):
    return jnp.where(seeds == 1, 1.0, jnp.where(irreversible == 1, old, 0.0))


def clamp(damage, update, lower_bound):
    return jnp.minimum(jnp.maximum(damage + update, lower_bound), 1.0)


def first_kernel(
    energy_hbm, old_hbm, seeds_hbm, irreversible_hbm, inverses_hbm,
    out_ref, high_ref, low_ref, ends_ref,
    energy_ref, old_ref, seeds_ref, irreversible_ref, inverses_ref, flat_refs, sems,
):
    pairs = [
        (old_hbm, old_ref), (seeds_hbm, seeds_ref), (irreversible_hbm, irreversible_ref),
        (energy_hbm, energy_ref), (inverses_hbm, inverses_ref),
    ]
    copies = [pltpu.make_async_copy(src, dst, sems.at[i]) for i, (src, dst) in enumerate(pairs)]
    for copy in copies:
        copy.start()
    for copy in copies[:4]:
        copy.wait()
    damage = jnp.where(seeds_ref[0] == 1, 1.0, old_ref[0])
    lower = bound(old_ref[0], seeds_ref[0], irreversible_ref[0])
    energy = energy_ref[0]
    partial_value = energy - (1.0 + energy) * damage + KAPPA * lane_lap(damage)
    send_pair(out_ref, flat_refs.at[0], jnp.concatenate(swap(odd_rows(), damage, lower), axis=0), 4, 10)
    copies[4].wait()
    send_single(out_ref, flat_refs.at[1], energy, 8, 10)
    split_inverses(inverses_ref, high_ref, low_ref, ends_ref)
    solved = line_solve(jnp.concatenate([partial_value, damage], axis=0), high_ref, low_ref, ends_ref)
    count = damage.shape[0]
    stacked = jnp.concatenate(swap(odd_rows(), solved[:count], solved[count:]), axis=0)
    send_pair(out_ref, flat_refs.at[2], stacked, 0, 10)


def cross_kernel(in_ref, high_ref, low_ref, ends_ref, z_ref, out_ref, change_ref):
    z_inverse = z_ref[...]
    planes = z_inverse.shape[0]
    solved_part, solved_damage = gather_pair(in_ref, planes, 0, 10)
    turned = solved_part + KAPPA * (lane_lap(solved_damage) + plane_lap(solved_damage, planes))
    update = STEP * plane_mix(z_inverse, line_solve(turned, high_ref, low_ref, ends_ref))
    damage, lower = gather_pair(in_ref, planes, 4, 10)
    renewed = clamp(damage, update, lower)
    change_ref[...] = jnp.full(change_ref.shape, jnp.sum((renewed - damage) ** 2), jnp.float32)
    energy = gather_single(in_ref, planes, 8, 10)
    partial_value = energy - (1.0 + energy) * renewed + KAPPA * (lane_lap(renewed) + plane_lap(renewed, planes))
    count = renewed.shape[0]
    solved = line_solve(jnp.concatenate([partial_value, renewed], axis=0), high_ref, low_ref, ends_ref)
    solved_part = plane_mix(z_inverse, solved[:count])
    solved_damage = plane_mix(z_inverse, solved[count:])
    steps = KAPPA * (solved_damage[planes:] - solved_damage[:-planes])
    rim = jnp.zeros((planes, solved.shape[1]), jnp.float32)
    solved_part = solved_part + jnp.concatenate([steps, rim], axis=0) - jnp.concatenate([rim, steps], axis=0)
    for i in range(4):
        part = slice(i * planes, (i + 1) * planes)
        scatter_row(out_ref, solved_part[part], renewed[part], planes, i, 5)
    scatter_row(out_ref, solved_damage[:planes], solved_damage[-planes:], planes, 4, 5)


def last_kernel(
    in_ref, old_ref, seeds_ref, irreversible_ref, high_ref, low_ref, ends_ref, first_change_ref,
    damage_ref, change_ref,
    flat_ref,
):
    chunks = in_ref.shape[0] // 5
    edges = in_ref[pl.ds(4, chunks, stride=5), :]
    inner = (low_half(chunks) != odd_rows()) & (iota((chunks, 128), 0) < chunks - 1)
    steps = pltpu.roll(edges, chunks - 1, 0) - pltpu.roll(edges, HALF, 1)
    steps = jnp.where(inner, KAPPA * steps, 0.0)
    for i in range(4):
        value = in_ref[pl.ds(i, chunks, stride=5), :]
        if i == 0:
            value = value - pltpu.roll(steps, 1, 0)
        if i == 3:
            value = value + steps
        flat_ref[pl.ds(i, chunks, stride=4), :] = value
    tiles = [flat_ref[t : t + 128, :].T for t in range(0, 4 * chunks, 128)]
    turned = jnp.concatenate([tile[:HALF] for tile in tiles], axis=1)
    damage = jnp.concatenate([tile[HALF:] for tile in tiles], axis=1)
    turned, damage = swap(odd_rows(), turned, damage)
    update = STEP * line_solve(turned, high_ref, low_ref, ends_ref)
    renewed = clamp(damage, update, bound(old_ref[0], seeds_ref[0], irreversible_ref[0]))
    damage_ref[0] = renewed
    change = jnp.sum((renewed - damage) ** 2)
    lane = iota(change_ref.shape, 1)
    change_ref[...] = jnp.where(lane == 0, first_change_ref[...], jnp.where(lane == 1, change, 0.0))


def call(kernel, outs, *args, direct=True, scratch=()):
    space = pltpu.VMEM if direct else pl.ANY
    if not direct:
        args = [pltpu.with_memory_space_constraint(arg, pltpu.HBM) for arg in args]
    return pl.pallas_call(
        kernel,
        out_shape=[pltpu.VMEM(shape, dtype) for shape, dtype in outs],
        in_specs=[pl.BlockSpec(memory_space=space) for _ in args],
        out_specs=[pl.BlockSpec(memory_space=pltpu.VMEM) for _ in outs],
        scratch_shapes=scratch,
        compiler_params=pltpu.CompilerParams(vmem_limit_bytes=20 * 1024 * 1024),
    )(*args)


def exchange(rows, axes):
    return lax.all_to_all(rows, axes, split_axis=0, concat_axis=0, tiled=True)


def cross(rows):
    return exchange(rows.reshape(-1, 1, 128), ALL).reshape(rows.shape)


def local(energy, damage_old, crack_seeds, irreversible, line_inverses, z_inverse):
    planes, rows_here, line_length = energy.shape
    cell_count = planes * rows_here * line_length * lax.axis_size(ALL)
    one = planes * rows_here * line_length // 128
    inputs = (energy, damage_old, crack_seeds, irreversible, line_inverses)
    scratch = [pltpu.VMEM(part.shape, part.dtype) for part in inputs]
    scratch += [pltpu.VMEM((3, 2 * one, 128), jnp.float32), pltpu.SemaphoreType.DMA((5,))]
    f32, bf16 = jnp.float32, jnp.bfloat16
    blocks, cells, _ = line_inverses.shape
    sent, *split = call(
        first_kernel,
        [((5 * one, 128), f32), (line_inverses.shape, bf16), (line_inverses.shape, bf16), ((blocks, 8, cells), f32)],
        *inputs,
        direct=False,
        scratch=scratch,
    )
    sent, change = call(
        cross_kernel, [((5 * one // 2, 128), f32), ((1, 128), f32)], cross(sent), *split, z_inverse
    )
    damage, change = call(
        last_kernel,
        [(energy.shape, f32), ((lax.axis_size(PLANE), 128), f32)],
        cross(sent),
        damage_old,
        crack_seeds,
        irreversible,
        *split,
        change,
        scratch=[pltpu.VMEM((2 * one, 128), f32)],
    )
    plane_sums = jnp.sum(exchange(change, PLANE), axis=0, keepdims=True)
    every = exchange(jnp.broadcast_to(plane_sums, (lax.axis_size(ROW[0]), 128)), ROW[:1])
    global_sums = jnp.sum(every, axis=0)[:ITERS]
    update_norms = jnp.sqrt(global_sums / cell_count + EPSILON) / STEP
    return (damage, update_norms)


def solution(mesh):
    finer = Mesh(mesh.devices.reshape(8, 2, 2, 4, 4), ALL)
    spec = P(COL, ROW, None)
    in_specs = (spec, spec, spec, spec, P(), P())
    return jax.shard_map(local, mesh=finer, in_specs=in_specs, out_specs=(spec, P()), check_vma=False)
```

```python
import jax
import jax.numpy as jnp
from jax import lax
from jax.experimental import pallas as pl
from jax.experimental.pallas import tpu as pltpu
from jax.sharding import Mesh
from jax.sharding import PartitionSpec as P

ROW = ("row_0", "row_1", "row_2")
COL = ("col_0", "col_1")
ALL = ROW + COL
PLANE = ROW[1:] + COL
CROSS = ROW[:-1] + COL + ROW[-1:]

ITERS = 2

KAPPA = 2.0
STEP = 0.02
COUPLE = 0.5
EPSILON = 1e-06
HALF = 64


def iota(shape, axis):
    return lax.broadcasted_iota(jnp.int32, shape, axis)


def lane_lap(field):
    extent = field.shape[1]
    lane = iota(field.shape, 1)
    ahead = jnp.where(lane == extent - 1, field, pltpu.roll(field, extent - 1, 1))
    behind = jnp.where(lane == 0, field, pltpu.roll(field, 1, 1))
    return (ahead - field) + (behind - field)


def plane_lap(field, planes):
    extent = field.shape[0]
    plane = iota(field.shape, 0) % planes
    ahead = jnp.where(plane == planes - 1, field, pltpu.roll(field, extent - 1, 0))
    behind = jnp.where(plane == 0, field, pltpu.roll(field, 1, 0))
    return (ahead - field) + (behind - field)


def halves(value):
    high = value.astype(jnp.bfloat16)
    return high, (value - high.astype(jnp.float32)).astype(jnp.bfloat16)


def product(rows, high, low, dims):
    count = rows.shape[0]
    rows_high, rows_low = halves(rows)
    both = lax.dot_general(
        jnp.concatenate([rows_high, rows_low], axis=0), high, (dims, ((), ())), preferred_element_type=jnp.float32
    )
    rest = lax.dot_general(rows_high, low, (dims, ((), ())), preferred_element_type=jnp.float32)
    return both[:count] + both[count:] + rest


def split_inverses(inverses_ref, high_ref, low_ref, ends_ref):
    blocks, cells, _ = inverses_ref.shape
    unit_row = iota((16, cells), 0)
    unit_lane = iota((16, cells), 1)
    units = jnp.where(
        ((unit_row == 0) & (unit_lane == 0)) | ((unit_row == 1) & (unit_lane == cells - 1)), 1.0, 0.0
    ).astype(jnp.bfloat16)
    for k in range(blocks):
        high, low = halves(inverses_ref[k])
        high_ref[k] = high
        low_ref[k] = low
        dims = (((1,), (1,)), ((), ()))
        ends = lax.dot_general(units, high, dims, preferred_element_type=jnp.float32) + lax.dot_general(
            units, low, dims, preferred_element_type=jnp.float32
        )
        ends_ref[k] = ends[:8]
        ends_ref[k, 2:3, :] = jnp.broadcast_to(ends[0:1, 0:1], (1, cells))
        ends_ref[k, 3:4, :] = jnp.broadcast_to(ends[0:1, cells - 1 : cells], (1, cells))
        ends_ref[k, 4:5, :] = jnp.broadcast_to(ends[1:2, 0:1], (1, cells))


def line_solve(lines, high_ref, low_ref, ends_ref):
    count = lines.shape[0]
    blocks, cells, _ = high_ref.shape
    products, firsts, lasts = [], [], []
    for k in range(blocks):
        products.append(product(lines[:, k * cells : (k + 1) * cells], high_ref[k], low_ref[k], ((1,), (1,))))
        firsts.append(ends_ref[k, 0:1, :])
        lasts.append(ends_ref[k, 1:2, :])
    wide = (count, 128)
    inflow, outflow = [None], [None] * blocks
    heads = [jnp.broadcast_to(products[0][:, 0:1], wide)]
    carried = jnp.broadcast_to(products[0][:, cells - 1 : cells], wide)
    for k in range(1, blocks):
        inflow.append(COUPLE * carried)
        heads.append(jnp.broadcast_to(products[k][:, 0:1], wide) + inflow[k] * ends_ref[k, 2:3, :128])
        if k < blocks - 1:
            carried = (
                jnp.broadcast_to(products[k][:, cells - 1 : cells], wide) + inflow[k] * ends_ref[k, 3:4, :128]
            )
    carried = heads[blocks - 1]
    for k in range(blocks - 2, -1, -1):
        outflow[k] = COUPLE * carried
        carried = heads[k] + outflow[k] * ends_ref[k, 4:5, :128]
    solved = []
    for k in range(blocks):
        for half in range(0, cells, 128):
            value = products[k][:, half : half + 128]
            if k > 0:
                value = value + inflow[k] * firsts[k][:, half : half + 128]
            if k < blocks - 1:
                value = value + outflow[k] * lasts[k][:, half : half + 128]
            solved.append(value)
    return jnp.concatenate(solved, axis=1)


def low_half(count):
    return iota((count, 2 * HALF), 1) < HALF


def odd_rows():
    return lax.axis_index(ROW[-1]) == 1


def swap(odd, one, two):
    return jnp.where(odd, two, one), jnp.where(odd, one, two)


def send_pair(out_ref, flat_ref, stacked, first, stride):
    chunks = out_ref.shape[0] // stride
    for t in range(0, 4 * chunks, 128):
        flat_ref[t : t + 128, :] = stacked[:, t : t + 128].T
    for i in range(4):
        out_ref[pl.ds(first + i, chunks, stride=stride), :] = flat_ref[pl.ds(i, chunks, stride=4), :]


def send_single(out_ref, flat_ref, field, first, stride):
    chunks = out_ref.shape[0] // stride
    doubled = jnp.concatenate([field, field], axis=0)
    for t in range(0, 4 * chunks, 128):
        flat_ref[t : t + 128, :] = doubled[:, t : t + 128].T
    for i in range(2):
        out_ref[pl.ds(first + i, chunks, stride=stride), :] = jnp.where(
            low_half(chunks) != odd_rows(),
            flat_ref[pl.ds(i, chunks, stride=4), :],
            flat_ref[pl.ds(i + 2, chunks, stride=4), :],
        )


def gather_row(in_ref, planes, at, stride):
    rows = in_ref.shape[0] // (stride * planes)
    low = low_half(planes)
    ones, twos = [], []
    for j in range(rows // 2):
        top = 2 * j * stride * planes + at
        even = in_ref[pl.ds(top, planes, stride=2 * stride), :]
        odd = in_ref[pl.ds(top + stride, planes, stride=2 * stride), :]
        ones.append(jnp.where(low, even, odd))
        twos.append(pltpu.roll(jnp.where(low, odd, even), HALF, 1))
    return jnp.concatenate(ones, axis=1), jnp.concatenate(twos, axis=1)


def scatter_row(out_ref, ones, twos, planes, at, stride):
    rows = out_ref.shape[0] // (stride * planes)
    low = low_half(planes)
    for j in range(rows // 2):
        one = ones[:, j * 128 : (j + 1) * 128]
        two = pltpu.roll(twos[:, j * 128 : (j + 1) * 128], HALF, 1)
        top = 2 * j * stride * planes + at
        out_ref[pl.ds(top, planes, stride=2 * stride), :] = jnp.where(
            low, one, two
        )
        out_ref[pl.ds(top + stride, planes, stride=2 * stride), :] = jnp.where(
            low, two, one
        )


def gather_pair(in_ref, planes, first, stride):
    pairs = [gather_row(in_ref, planes, first + i, stride) for i in range(4)]
    return [jnp.concatenate(part, axis=0) for part in zip(*pairs)]


def gather_single(in_ref, planes, first, stride):
    pairs = [gather_row(in_ref, planes, first + i, stride) for i in range(2)]
    return jnp.concatenate([part[half] for half in range(2) for part in pairs], axis=0)


def plane_mix(z_inverse, lines):
    planes = z_inverse.shape[0]
    copies = lines.shape[0] // planes
    tiled = jnp.concatenate([jnp.concatenate([z_inverse] * copies, axis=1)] * copies, axis=0)
    same = iota(tiled.shape, 0) // planes == iota(tiled.shape, 1) // planes
    high, low = halves(lines)
    return product(jnp.where(same, tiled, 0.0), high, low, ((1,), (0,)))


def bound(old, seeds, irreversible):
    return jnp.where(seeds == 1, 1.0, jnp.where(irreversible == 1, old, 0.0))


def clamp(damage, update, lower_bound):
    return jnp.minimum(jnp.maximum(damage + update, lower_bound), 1.0)


def first_kernel(
    energy_hbm, old_hbm, seeds_hbm, irreversible_hbm, inverses_hbm,
    out_ref, high_ref, low_ref, ends_ref,
    energy_ref, old_ref, seeds_ref, irreversible_ref, inverses_ref, flat_refs, sems,
):
    pairs = [
        (old_hbm, old_ref), (seeds_hbm, seeds_ref), (irreversible_hbm, irreversible_ref),
        (energy_hbm, energy_ref), (inverses_hbm, inverses_ref),
    ]
    copies = [pltpu.make_async_copy(src, dst, sems.at[i]) for i, (src, dst) in enumerate(pairs)]
    for copy in copies:
        copy.start()
    for copy in copies[:4]:
        copy.wait()
    damage = jnp.where(seeds_ref[0] == 1, 1.0, old_ref[0])
    lower = bound(old_ref[0], seeds_ref[0], irreversible_ref[0])
    energy = energy_ref[0]
    partial_value = energy - (1.0 + energy) * damage + KAPPA * lane_lap(damage)
    send_pair(out_ref, flat_refs.at[0], jnp.concatenate(swap(odd_rows(), damage, lower), axis=0), 4, 10)
    copies[4].wait()
    send_single(out_ref, flat_refs.at[1], energy, 8, 10)
    split_inverses(inverses_ref, high_ref, low_ref, ends_ref)
    solved = line_solve(jnp.concatenate([partial_value, damage], axis=0), high_ref, low_ref, ends_ref)
    count = damage.shape[0]
    stacked = jnp.concatenate(swap(odd_rows(), solved[:count], solved[count:]), axis=0)
    send_pair(out_ref, flat_refs.at[2], stacked, 0, 10)


def cross_kernel(in_ref, high_ref, low_ref, ends_ref, z_ref, out_ref, change_ref):
    z_inverse = z_ref[...]
    planes = z_inverse.shape[0]
    solved_part, solved_damage = gather_pair(in_ref, planes, 0, 10)
    turned = solved_part + KAPPA * (lane_lap(solved_damage) + plane_lap(solved_damage, planes))
    update = STEP * plane_mix(z_inverse, line_solve(turned, high_ref, low_ref, ends_ref))
    damage, lower = gather_pair(in_ref, planes, 4, 10)
    renewed = clamp(damage, update, lower)
    change_ref[...] = jnp.full(change_ref.shape, jnp.sum((renewed - damage) ** 2), jnp.float32)
    energy = gather_single(in_ref, planes, 8, 10)
    partial_value = energy - (1.0 + energy) * renewed + KAPPA * (lane_lap(renewed) + plane_lap(renewed, planes))
    count = renewed.shape[0]
    solved = line_solve(jnp.concatenate([partial_value, renewed], axis=0), high_ref, low_ref, ends_ref)
    solved_part = plane_mix(z_inverse, solved[:count])
    solved_damage = plane_mix(z_inverse, solved[count:])
    steps = KAPPA * (solved_damage[planes:] - solved_damage[:-planes])
    rim = jnp.zeros((planes, solved.shape[1]), jnp.float32)
    solved_part = solved_part + jnp.concatenate([steps, rim], axis=0) - jnp.concatenate([rim, steps], axis=0)
    for i in range(4):
        part = slice(i * planes, (i + 1) * planes)
        scatter_row(out_ref, solved_part[part], renewed[part], planes, i, 5)
    scatter_row(out_ref, solved_damage[:planes], solved_damage[-planes:], planes, 4, 5)


def last_kernel(
    in_ref, old_ref, seeds_ref, irreversible_ref, high_ref, low_ref, ends_ref, first_change_ref,
    damage_ref, change_ref,
    flat_ref,
):
    chunks = in_ref.shape[0] // 5
    edges = in_ref[pl.ds(4, chunks, stride=5), :]
    inner = (low_half(chunks) != odd_rows()) & (iota((chunks, 128), 0) < chunks - 1)
    steps = pltpu.roll(edges, chunks - 1, 0) - pltpu.roll(edges, HALF, 1)
    steps = jnp.where(inner, KAPPA * steps, 0.0)
    for i in range(4):
        value = in_ref[pl.ds(i, chunks, stride=5), :]
        if i == 0:
            value = value - pltpu.roll(steps, 1, 0)
        if i == 3:
            value = value + steps
        flat_ref[pl.ds(i, chunks, stride=4), :] = value
    tiles = [flat_ref[t : t + 128, :].T for t in range(0, 4 * chunks, 128)]
    turned = jnp.concatenate([tile[:HALF] for tile in tiles], axis=1)
    damage = jnp.concatenate([tile[HALF:] for tile in tiles], axis=1)
    turned, damage = swap(odd_rows(), turned, damage)
    update = STEP * line_solve(turned, high_ref, low_ref, ends_ref)
    renewed = clamp(damage, update, bound(old_ref[0], seeds_ref[0], irreversible_ref[0]))
    damage_ref[0] = renewed
    change = jnp.sum((renewed - damage) ** 2)
    lane = iota(change_ref.shape, 1)
    change_ref[...] = jnp.where(lane == 0, first_change_ref[...], jnp.where(lane == 1, change, 0.0))


def call(kernel, outs, *args, direct=True, scratch=()):
    space = pltpu.VMEM if direct else pl.ANY
    if not direct:
        args = [pltpu.with_memory_space_constraint(arg, pltpu.HBM) for arg in args]
    return pl.pallas_call(
        kernel,
        out_shape=[pltpu.VMEM(shape, dtype) for shape, dtype in outs],
        in_specs=[pl.BlockSpec(memory_space=space) for _ in args],
        out_specs=[pl.BlockSpec(memory_space=pltpu.VMEM) for _ in outs],
        scratch_shapes=scratch,
        compiler_params=pltpu.CompilerParams(vmem_limit_bytes=20 * 1024 * 1024),
    )(*args)


def exchange(rows, axes):
    return lax.all_to_all(rows, axes, split_axis=0, concat_axis=0, tiled=True)


def cross(rows):
    return exchange(rows.reshape(-1, 1, 128), CROSS).reshape(rows.shape)


def local(energy, damage_old, crack_seeds, irreversible, line_inverses, z_inverse):
    planes, rows_here, line_length = energy.shape
    cell_count = planes * rows_here * line_length * lax.axis_size(ALL)
    one = planes * rows_here * line_length // 128
    inputs = (energy, damage_old, crack_seeds, irreversible, line_inverses)
    scratch = [pltpu.VMEM(part.shape, part.dtype) for part in inputs]
    scratch += [pltpu.VMEM((3, 2 * one, 128), jnp.float32), pltpu.SemaphoreType.DMA((5,))]
    f32, bf16 = jnp.float32, jnp.bfloat16
    blocks, cells, _ = line_inverses.shape
    sent, *split = call(
        first_kernel,
        [((5 * one, 128), f32), (line_inverses.shape, bf16), (line_inverses.shape, bf16), ((blocks, 8, cells), f32)],
        *inputs,
        direct=False,
        scratch=scratch,
    )
    sent, change = call(
        cross_kernel, [((5 * one // 2, 128), f32), ((1, 128), f32)], cross(sent), *split, z_inverse
    )
    damage, change = call(
        last_kernel,
        [(energy.shape, f32), ((lax.axis_size(PLANE), 128), f32)],
        cross(sent),
        damage_old,
        crack_seeds,
        irreversible,
        *split,
        change,
        scratch=[pltpu.VMEM((2 * one, 128), f32)],
    )
    plane_sums = jnp.sum(exchange(change, PLANE), axis=0, keepdims=True)
    every = exchange(jnp.broadcast_to(plane_sums, (lax.axis_size(ROW[0]), 128)), ROW[:1])
    global_sums = jnp.sum(every, axis=0)[:ITERS]
    update_norms = jnp.sqrt(global_sums / cell_count + EPSILON) / STEP
    return (damage, update_norms)


def solution(mesh):
    finer = Mesh(mesh.devices.reshape(8, 2, 2, 4, 4), ALL)
    spec = P(COL, ROW, None)
    in_specs = (spec, spec, spec, spec, P(), P())
    return jax.shard_map(local, mesh=finer, in_specs=in_specs, out_specs=(spec, P()), check_vma=False)
```
